256 devices in a mesh: slides: 2 (over y), row: 128 (over x, z, core).
Axes of the slice: x: 4, y: 2, z: 16, core: 2. Of those that a mesh axis runs over, the one named last changes fastest.
The devices are a block of a 4x16x16 slice.
Arguments:
- slide_pixels: bfloat16 [16384, 16384], P(('slides', 'row')), parts along dimension 0, may hold values from -6 to 6
- tissue_mask: int32 [512, 8], P(('slides', 'row')), parts along dimension 0, may hold values from 0 to 1, as said below
- conv_weight: bfloat16 [3, 3, 64, 64], replicated, may hold values from -0.25 to 0.25
- conv_bias: bfloat16 [64], replicated, may hold values from -3 to 3
Outputs:
- packed_tiles: bfloat16 [2048, 32, 2048], P(('slides', 'row')), parts along dimension 0
The draws below stay inside these ranges and needn't reach their ends.
There are 2 independent parts, one for each index of `slides`. The reference program is written for one: setup_inputs(seed, part) draws one part's arguments, and reference() takes and returns one part's arrays. A program takes and returns all parts, laid end to end along the dimension named above; an argument that names none is the same for every part. Nothing has to cross between parts.
Inputs may be any that keep to these rules, and one draw needn't show every extreme that they name: `tissue_mask`: exactly 1024 tiles hold tissue. For every s from 1 to 127, the first s * 2 tile rows hold s * 8 + e tissue tiles with e between 0 and 2; e = 2 occurs in every draw. For every such s, some column holds tissue in both tile row s * 2 - 1 and tile row s * 2.
All inputs are finite; a program needn't handle non-finite values.
Results may differ from the reference program's by a relative error of at most 0.001.
Values may be sent and summed in bfloat16 or wider, within the bound.
No kernel may reach another device: no remote copies, remote signals or barrier semaphores. Data moves between devices by JAX's collectives and lax.ppermute only.
A program may use at most 64 MiB of HBM per device.

```python
import jax
import jax.numpy as jnp
from jax import lax

CH = 64
SIDE = 32
SLOTS = 8
ROWS_DEV = 2
COLS = 8
SHIFT_MOST = 2
GRID_ROWS = 256
N_ROW = 128


def draw_tissue_mask(key, part):
    walk_key, first_key, order_key, column_key = jax.random.split(jax.random.fold_in(key, 7), 4)
    device_total = N_ROW
    reach_most = SHIFT_MOST
    drift_walk = jax.random.randint(walk_key, (device_total + 1,), 0, reach_most + 1)
    first_step = jax.random.randint(first_key, (), 1, device_total)
    step_index = jnp.arange(device_total + 1)
    drift_walk = jnp.where(step_index == first_step, reach_most, drift_walk)
    middle = device_total // 2
    in_window = (step_index >= middle - 2) & (step_index <= middle + 3)
    alternating = step_index % 2 * reach_most
    drift_walk = jnp.where(in_window, alternating, drift_walk)
    drift_walk = jnp.where((step_index == 0) | (step_index == device_total), 0, drift_walk)
    counts = SLOTS + drift_walk[1:] - drift_walk[:-1]
    tiles_band = ROWS_DEV * COLS
    boundary_cols = jax.random.randint(column_key, (device_total + 1,), 0, COLS)
    tile_index = jnp.arange(tiles_band)
    top_forced = tile_index[None, :] == boundary_cols[:-1, None]
    bottom_forced = tile_index[None, :] == (ROWS_DEV - 1) * COLS + boundary_cols[1:, None]
    band_index = jnp.arange(device_total)[:, None]
    forced = top_forced & (band_index > 0) | bottom_forced & (band_index < device_total - 1)
    scores = jax.random.randint(order_key, (device_total, tiles_band), 0, 1 << 20) * tiles_band
    scores = scores + tile_index[None, :]
    scores = jnp.where(forced, -1 - tile_index[None, :], scores)
    ranking = jnp.argsort(jnp.argsort(scores, axis=1), axis=1)
    tissue = (ranking < counts[:, None]).astype(jnp.int32)
    return tissue.reshape(device_total * ROWS_DEV, COLS)


def steps_of(key, dims, cuts, smallest, largest):
    loudness, own = 1.0, jax.random.fold_in(key, 6)
    for dim, parts in cuts:
        steps = jnp.exp(jax.random.uniform(jax.random.fold_in(own, dim), (parts,), jnp.float32, smallest / len(cuts), largest / len(cuts)))
        loudness = loudness * jnp.repeat(steps, dims[dim] // parts).reshape([-1 if axis == dim else 1 for axis in range(len(dims))])
    return loudness


def noise(stream_key, extent, width, bound, cuts=(), held_as=jnp.bfloat16):
    loudness = steps_of(stream_key, extent, cuts, -0.22, 0.18) if cuts else 1.0
    array = jax.random.normal(stream_key, extent, jnp.float32) * width * loudness
    return jnp.minimum(jnp.maximum(array, -bound), bound).astype(held_as)


def setup_inputs(seed: int = 0, part: int = 0) -> dict:
    key_of = jax.random.split(jax.random.key(seed), 5)
    own_keys = jax.random.split(jax.random.fold_in(key_of[4], part), 5)
    slide_pixels = noise(own_keys[0], (GRID_ROWS * SIDE, COLS * SIDE * CH), 1.0, 6.0, ((0, 128),))
    tissue_mask = draw_tissue_mask(jax.random.fold_in(jax.random.fold_in(key_of[4], part), 71), part)
    conv_weight = noise(key_of[2], (3, 3, CH, CH), (9 * CH) ** -0.5, 0.25)
    conv_bias = noise(key_of[3], (CH,), 0.5, 3.0)
    return dict(slide_pixels=slide_pixels, tissue_mask=tissue_mask, conv_weight=conv_weight, conv_bias=conv_bias)


def reference(slide_pixels, tissue_mask, conv_weight, conv_bias):
    grid_rows, grid_cols = tissue_mask.shape
    channels = conv_weight.shape[2]
    side = slide_pixels.shape[0] // grid_rows
    image = slide_pixels.reshape(grid_rows * side, grid_cols * side, channels)
    flat_mask = tissue_mask.reshape(grid_rows * grid_cols)
    order = jnp.argsort(1 - flat_mask, stable=True)[: N_ROW * SLOTS].astype(jnp.int32)
    weight_full = conv_weight.astype(jnp.float32)
    bias_full = conv_bias.astype(jnp.float32)

    def one_tile(position):
        tile_row = position // grid_cols
        tile_col = position % grid_cols
        offsets = jnp.arange(side + 2, dtype=jnp.int32) - 1
        pixel_rows = tile_row * side + offsets
        pixel_cols = tile_col * side + offsets
        row_inside = (pixel_rows >= 0) & (pixel_rows < grid_rows * side)
        col_inside = (pixel_cols >= 0) & (pixel_cols < grid_cols * side)
        rows_safe = jnp.clip(pixel_rows, 0, grid_rows * side - 1).astype(jnp.int32)
        cols_safe = jnp.clip(pixel_cols, 0, grid_cols * side - 1).astype(jnp.int32)
        window = jnp.take(jnp.take(image, rows_safe, axis=0), cols_safe, axis=1).astype(jnp.float32)
        tissue = jnp.take(jnp.take(tissue_mask, rows_safe // side, axis=0), cols_safe // side, axis=1)
        living = row_inside[:, None] & col_inside[None, :] & (tissue == 1)
        window = jnp.where(living[:, :, None], window, jnp.zeros_like(window))
        result = jnp.zeros((side, side, channels), jnp.float32)
        for vertical in range(3):
            for horizontal in range(3):
                result = result + jnp.einsum(
                    "hwc,co->hwo",
                    window[vertical:vertical + side, horizontal:horizontal + side],
                    weight_full[vertical, horizontal],
                    precision=lax.Precision.HIGHEST)
        result = result + bias_full
        return result.astype(jnp.bfloat16).reshape(side, side * channels)

    return lax.map(one_tile, order)
```

```python
import functools

import jax
import jax.numpy as jnp
from jax import lax
from jax.experimental import pallas as pl
from jax.experimental.pallas import tpu as pltpu
from jax.sharding import PartitionSpec as P

SLOTS = 8
SHIFT_MOST = 2
LANES = 128
GUARD = 16


def edge_kernel(mask, first_rows, last_rows, first, last, *, grid_cols, tile_lanes):
    for col in range(grid_cols):
        lanes = pl.ds(col * tile_lanes, tile_lanes)
        top = first_rows[0:1, lanes]
        first[:, lanes] = jnp.where(mask[0, col] == 1, top, jnp.zeros_like(top))
        low = last_rows[last_rows.shape[0] - 1 :, lanes]
        last[:, lanes] = jnp.where(mask[1, col] == 1, low, jnp.zeros_like(low))


def edges(mask, pixels):
    band, width = pixels.shape
    grid_cols = mask.shape[1]
    step = 16
    row = jax.ShapeDtypeStruct((1, width), pixels.dtype)
    whole = pl.BlockSpec((1, width), lambda i: (0, 0))
    return pl.pallas_call(
        functools.partial(edge_kernel, grid_cols=grid_cols, tile_lanes=width // grid_cols),
        grid=(1,),
        in_specs=[
            pl.BlockSpec(memory_space=pltpu.SMEM),
            pl.BlockSpec((step, width), lambda i: (0, 0)),
            pl.BlockSpec((step, width), lambda i: (band // step - 1, 0)),
        ],
        out_specs=[whole, whole],
        out_shape=[row, row],
    )(mask, pixels, pixels)


def conv_kernel(
    mask, pixels, above, below, weight, bias, tiles, tail,
    band, shifted, banded, made, in_sem, out_sem, tail_sem,
    *, rows, cols, side, ch,
):
    wide = side * ch
    count = rows * cols

    def tissue(t):
        return mask[t // cols, t % cols]

    def fetch(t):
        row, col = t // cols, t % cols
        return pltpu.make_async_copy(
            pixels.at[pl.ds(row * side, side), pl.ds(col * wide, wide)],
            band.at[pl.ds(GUARD + row * side, side), pl.ds(LANES + col * wide, wide)],
            in_sem.at[t],
        )

    for t in range(count):
        row, col = t // cols, t % cols

        @pl.when(tissue(t) == 1)
        def _():
            fetch(t).start()

        @pl.when(tissue(t) != 1)
        def _():
            band[GUARD + row * side : GUARD + (row + 1) * side, LANES + col * wide : LANES + (col + 1) * wide] = (
                jnp.zeros((side, wide), band.dtype)
            )

    edge = jnp.zeros((band.shape[0], LANES), band.dtype)
    band[:, 0:LANES] = edge
    band[:, LANES + cols * wide :] = edge
    inner = pl.ds(LANES, cols * wide)
    band[0:GUARD, inner] = jnp.broadcast_to(above[...], (GUARD, cols * wide))
    band[GUARD + rows * side :, inner] = jnp.broadcast_to(below[...], (GUARD, cols * wide))

    spread = lax.broadcasted_iota(jnp.int32, (ch, 2 * ch), 1) - lax.broadcasted_iota(jnp.int32, (ch, 2 * ch), 0)
    taps = weight[...]
    halves = [
        jnp.dot(taps, (spread == at * ch).astype(taps.dtype), preferred_element_type=jnp.float32).astype(taps.dtype)
        for at in range(2)
    ]
    for v in range(3):
        left, right = (h[3 * v * ch : 3 * (v + 1) * ch] for h in halves)
        base = 4 * v * ch
        banded[base : base + ch] = left[0:ch]
        banded[base + ch : base + 3 * ch] = left[ch:] + right[: 2 * ch]
        banded[base + 3 * ch : base + 4 * ch] = right[2 * ch :]

    for t in range(count):

        @pl.when(tissue(t) == 1)
        def _():
            fetch(t).wait()

    total = sum(tissue(t) for t in range(count))

    def store(t, at):
        return pltpu.make_async_copy(made.at[at], tiles.at[at], out_sem.at[t])

    def hand_on(t, at):
        return pltpu.make_async_copy(made.at[at], tail.at[at - (total - SHIFT_MOST)], tail_sem.at[t])

    def each(t, at):
        live = tissue(t) == 1

        @pl.when(live)
        def _():
            row, col = t // cols, t % cols
            window = band[
                pl.ds(pl.multiple_of(row * side, GUARD), side + 2 * GUARD),
                pl.ds(pl.multiple_of(col * wide, LANES), wide + 2 * LANES),
            ].astype(jnp.float32)
            window = window[:, LANES // 2 : LANES // 2 + wide + LANES]
            for v in range(3):
                shifted[v] = window[GUARD + v - 1 : GUARD + v - 1 + side].astype(band.dtype)
            pairs = wide // LANES
            total_rows = None
            for v in range(3):
                left = jnp.concatenate([shifted[v, :, p * LANES : p * LANES + 2 * LANES] for p in range(pairs)], axis=0)
                part = jnp.dot(left, banded[4 * v * ch : 4 * (v + 1) * ch], preferred_element_type=jnp.float32)
                total_rows = part if total_rows is None else total_rows + part
            result = (total_rows + bias[...]).astype(band.dtype)
            for p in range(pairs):
                made[at, :, p * LANES : (p + 1) * LANES] = result[p * side : (p + 1) * side]
            store(t, at).start()

            @pl.when(at >= total - SHIFT_MOST)
            def _():
                hand_on(t, at).start()

        return at + tissue(t)

    lax.fori_loop(0, count, each, jnp.int32(0))

    def finish(t, at):
        @pl.when(tissue(t) == 1)
        def _():
            store(t, at).wait()

            @pl.when(at >= total - SHIFT_MOST)
            def _():
                hand_on(t, at).wait()

        return at + tissue(t)

    lax.fori_loop(0, count, finish, jnp.int32(0))


def convolve(mask, pixels, above, below, weight, bias):
    rows, cols = mask.shape
    side = pixels.shape[0] // rows
    ch = weight.shape[2]
    wide = side * ch
    most = SLOTS + SHIFT_MOST
    dtype = pixels.dtype
    smem = pl.BlockSpec(memory_space=pltpu.SMEM)
    vmem = pl.BlockSpec(memory_space=pltpu.VMEM)
    hbm = pl.BlockSpec(memory_space=pl.ANY)
    return pl.pallas_call(
        functools.partial(conv_kernel, rows=rows, cols=cols, side=side, ch=ch),
        in_specs=[smem, hbm, vmem, vmem, vmem, vmem],
        out_specs=[hbm, hbm],
        out_shape=[
            jax.ShapeDtypeStruct((most, side, wide), dtype),
            jax.ShapeDtypeStruct((SHIFT_MOST, side, wide), dtype),
        ],
        scratch_shapes=[
            pltpu.VMEM((rows * side + 2 * GUARD, cols * wide + 2 * LANES), dtype),
            pltpu.VMEM((3, side, wide + LANES), dtype),
            pltpu.VMEM((12 * ch, 2 * ch), dtype),
            pltpu.VMEM((most, side, wide), dtype),
            pltpu.SemaphoreType.DMA((rows * cols,)),
            pltpu.SemaphoreType.DMA((rows * cols,)),
            pltpu.SemaphoreType.DMA((rows * cols,)),
        ],
    )(
        mask,
        pixels,
        above,
        below,
        weight.reshape(9 * ch, ch),
        jnp.tile(bias.astype(jnp.float32), 2).reshape(1, 2 * ch),
    )


def place_kernel(excess, own, passed, out, sem):
    shift = excess[0]

    def copy_own(i):
        return pltpu.make_async_copy(own.at[i - shift], out.at[i], sem.at[i])

    def copy_passed(i):
        return pltpu.make_async_copy(passed.at[i + SHIFT_MOST - shift], out.at[i], sem.at[i])

    for act in ("start", "wait"):
        for i in range(out.shape[0]):
            if i < SHIFT_MOST:

                @pl.when(i < shift)
                def _():
                    getattr(copy_passed(i), act)()

                @pl.when(i >= shift)
                def _():
                    getattr(copy_own(i), act)()

            else:
                getattr(copy_own(i), act)()


def place(excess, own, passed):
    hbm = pl.BlockSpec(memory_space=pl.ANY)
    return pl.pallas_call(
        place_kernel,
        in_specs=[pl.BlockSpec(memory_space=pltpu.SMEM), hbm, hbm],
        out_specs=hbm,
        out_shape=jax.ShapeDtypeStruct((SLOTS,) + own.shape[1:], own.dtype),
        scratch_shapes=[pltpu.SemaphoreType.DMA((SLOTS,))],
    )(excess, own, passed)


def on_device(slide_pixels, tissue_mask, conv_weight, conv_bias):
    size = lax.axis_size("row")
    device = lax.axis_index("row")
    count = jnp.broadcast_to(jnp.sum(tissue_mask), (size, LANES))
    table = lax.all_to_all(count, "row", 0, 0, tiled=True)
    up = [(i, i + 1) for i in range(size - 1)]
    down = [(j, i) for i, j in up]
    first, last = edges(tissue_mask, slide_pixels)
    above = lax.ppermute(last, "row", up)
    below = lax.ppermute(first, "row", down)
    own, tail = convolve(tissue_mask, slide_pixels, above, below, conv_weight, conv_bias)
    passed = lax.ppermute(tail, "row", up)
    lower = jnp.arange(size, dtype=jnp.int32)[:, None] < device
    earlier = jnp.sum(jnp.where(lower, table, 0)[:, 0])
    excess = (earlier - device * SLOTS).astype(jnp.int32).reshape(1)
    return place(excess, own, passed)


def solution(mesh):
    spread = ("slides", "row")
    return jax.shard_map(
        on_device,
        mesh=mesh,
        in_specs=(P(spread, None), P(spread, None), P(), P()),
        out_specs=P(spread, None, None),
        check_vma=False,
    )
```

```python
import functools

import jax
import jax.numpy as jnp
from jax import lax
from jax.experimental import pallas as pl
from jax.experimental.pallas import tpu as pltpu
from jax.sharding import PartitionSpec as P

SLOTS = 8
SHIFT_MOST = 2
LANES = 128
GUARD = 16
RIM = 8


def fetch_band(mask, pixels, band, sem, *, rows, cols, side, wide, guard):
    def fetch(t):
        row, col = t // cols, t % cols
        return pltpu.make_async_copy(
            pixels.at[pl.ds(row * side, side), pl.ds(col * wide, wide)],
            band.at[pl.ds(guard + row * side, side), pl.ds(LANES + col * wide, wide)],
            sem.at[t],
        )

    for t in range(rows * cols):
        row, col = t // cols, t % cols

        @pl.when(mask[row, col] == 1)
        def _():
            fetch(t).start()

    for t in range(rows * cols):
        row, col = t // cols, t % cols

        @pl.when(mask[row, col] != 1)
        def _():
            band[guard + row * side : guard + (row + 1) * side, LANES + col * wide : LANES + (col + 1) * wide] = (
                jnp.zeros((side, wide), band.dtype)
            )

    edge = jnp.zeros((band.shape[0], LANES), band.dtype)
    band[:, 0:LANES] = edge
    band[:, LANES + cols * wide :] = edge

    def wait():
        for t in range(rows * cols):

            @pl.when(mask[t // cols, t % cols] == 1)
            def _():
                fetch(t).wait()

    return wait


def prepare_kernel(mask, pixels, card, first, last, parcel, band, sem, *, rows, cols, side, wide):
    count = rows * cols
    wait = fetch_band(mask, pixels, band, sem, rows=rows, cols=cols, side=side, wide=wide, guard=0)
    total = jnp.int32(0)
    for t in range(count):
        total = total + mask[t // cols, t % cols]
    places = []
    for k in range(SHIFT_MOST):
        rank, found = jnp.int32(0), jnp.int32(0)
        for t in range(count):
            hit = (mask[t // cols, t % cols] == 1) & (rank == total - SHIFT_MOST + k)
            found = jnp.where(hit, t, found)
            rank = rank + mask[t // cols, t % cols]
        places.append((found // cols, found % cols))
    lane = lax.broadcasted_iota(jnp.int32, card.shape, 2)
    info = jnp.where(lane == 0, total, 0)
    for k, (row, col) in enumerate(places):
        info = jnp.where(lane == 1 + 2 * k, row, jnp.where(lane == 2 + 2 * k, col, info))
    card[...] = info
    wait()
    first[...] = band[0:1, LANES : LANES + cols * wide]
    last[...] = band[rows * side - 1 :, LANES : LANES + cols * wide]
    window = wide + 2 * LANES
    line = lax.broadcasted_iota(jnp.int32, (RIM, window), 0)
    per = cols // SHIFT_MOST
    for k, (row, col) in enumerate(places):
        lanes = pl.ds(pl.multiple_of(col * wide, LANES), window)
        parcel[k, 0:side] = band[pl.ds(pl.multiple_of(row * side, side), side), lanes]
        near = band[pl.ds(pl.multiple_of(side - GUARD * row, GUARD), GUARD), lanes].astype(jnp.float32)
        rim = jnp.where(row == 0, near[0:1], near[GUARD - 1 : GUARD])
        block = jnp.broadcast_to(rim, (RIM, window))
        for j in range(per):
            at = (k * per + j) * wide
            low = band[rows * side - GUARD :, at : at + window].astype(jnp.float32)[GUARD - 1 : GUARD]
            block = jnp.where(line == 1 + j, jnp.broadcast_to(low, (RIM, window)), block)
        parcel[k, side:] = block.astype(parcel.dtype)


def prepare(mask, pixels, size):
    rows, cols = mask.shape
    side = pixels.shape[0] // rows
    wide = pixels.shape[1] // cols
    dtype = pixels.dtype
    vmem = pl.BlockSpec(memory_space=pltpu.VMEM)
    return pl.pallas_call(
        functools.partial(prepare_kernel, rows=rows, cols=cols, side=side, wide=wide),
        in_specs=[pl.BlockSpec(memory_space=pltpu.SMEM), pl.BlockSpec(memory_space=pl.ANY)],
        out_specs=[vmem, vmem, vmem, vmem],
        out_shape=[
            jax.ShapeDtypeStruct((size, 1, LANES), jnp.int32),
            jax.ShapeDtypeStruct((1, cols * wide), dtype),
            jax.ShapeDtypeStruct((1, cols * wide), dtype),
            jax.ShapeDtypeStruct((SHIFT_MOST, side + RIM, wide + 2 * LANES), dtype),
        ],
        scratch_shapes=[
            pltpu.VMEM((rows * side, cols * wide + 2 * LANES), dtype),
            pltpu.SemaphoreType.DMA((rows * cols,)),
        ],
    )(mask, pixels)


def conv_kernel(
    info, mask, pixels, parcel, farther, below, weight, bias, out,
    band, beyond, moved, shifted, banded, made, in_sem, out_sem,
    *, rows, cols, side, ch,
):
    wide = side * ch
    count = rows * cols
    window = wide + 2 * LANES
    slots = out.shape[0]
    excess = info[0]
    wait = fetch_band(mask, pixels, band, in_sem, rows=rows, cols=cols, side=side, wide=wide, guard=GUARD)

    per = cols // SHIFT_MOST
    for col in range(cols):
        row = parcel[col // per, side : side + RIM, LANES : LANES + wide].astype(jnp.float32)
        row = row[1 + col % per : 2 + col % per]
        at = LANES + col * wide
        band[0:GUARD, at : at + wide] = jnp.broadcast_to(row, (GUARD, wide)).astype(band.dtype)
    inner = pl.ds(LANES, cols * wide)
    band[GUARD + rows * side :, inner] = jnp.broadcast_to(below[...], (GUARD, cols * wide))
    beyond[:, inner] = jnp.broadcast_to(farther[...], (GUARD, cols * wide))
    edge = jnp.zeros((GUARD, LANES), band.dtype)
    beyond[:, 0:LANES] = edge
    beyond[:, LANES + cols * wide :] = edge

    spread = lax.broadcasted_iota(jnp.int32, (ch, 2 * ch), 1) - lax.broadcasted_iota(jnp.int32, (ch, 2 * ch), 0)
    taps = weight[...]
    halves = [
        jnp.dot(taps, (spread == at * ch).astype(taps.dtype), preferred_element_type=jnp.float32).astype(taps.dtype)
        for at in range(2)
    ]
    for v in range(3):
        left, right = (h[3 * v * ch : 3 * (v + 1) * ch] for h in halves)
        base = 4 * v * ch
        banded[base : base + ch] = left[0:ch]
        banded[base + ch : base + 3 * ch] = left[ch:] + right[: 2 * ch]
        banded[base + 3 * ch : base + 4 * ch] = right[2 * ch :]

    wait()

    for k in range(SHIFT_MOST):
        row, col = info[1 + 2 * k], info[2 + 2 * k]
        lanes = pl.ds(pl.multiple_of(col * wide, LANES), window)
        moved[k, GUARD : GUARD + side] = parcel[k, 0:side]
        rim = parcel[k, side : side + RIM].astype(jnp.float32)[0:1]
        rim = jnp.broadcast_to(rim, (GUARD, window)).astype(band.dtype)

        @pl.when(row == 0)
        def _():
            moved[k, 0:GUARD] = beyond[:, lanes]
            moved[k, GUARD + side :] = rim

        @pl.when(row != 0)
        def _():
            moved[k, 0:GUARD] = rim
            moved[k, GUARD + side :] = band[GUARD : 2 * GUARD, lanes]

    blocks = wide // LANES + 1

    def emit(source, slot):
        tile = source[:, LANES // 2 : LANES // 2 + blocks * LANES].astype(jnp.float32)
        for q in range(blocks):
            shifted[q] = tile[GUARD - RIM : GUARD + side + RIM, q * LANES : (q + 1) * LANES]
        result = None
        for v in range(3):
            start = RIM + v - 1
            part = [shifted[q, start : start + side].astype(band.dtype) for q in range(blocks)]
            left = jnp.concatenate(
                [jnp.concatenate([part[q], part[q + 1]], axis=1) for q in range(blocks - 1)], axis=0
            )
            term = jnp.dot(left, banded[4 * v * ch : 4 * (v + 1) * ch], preferred_element_type=jnp.float32)
            result = term if result is None else result + term
        result = (result + bias[...]).astype(band.dtype)
        for q in range(blocks - 1):
            made[slot, :, q * LANES : (q + 1) * LANES] = result[q * side : (q + 1) * side]
        pltpu.make_async_copy(made.at[slot], out.at[slot], out_sem.at[slot]).start()

    def own(t, rank):
        row, col = t // cols, t % cols
        slot = rank + excess

        @pl.when((mask[row, col] == 1) & (slot < slots))
        def _():
            emit(
                band[
                    pl.ds(pl.multiple_of(row * side, GUARD), side + 2 * GUARD),
                    pl.ds(pl.multiple_of(col * wide, LANES), window),
                ],
                slot,
            )

        return rank + mask[row, col]

    lax.fori_loop(0, count, own, jnp.int32(0))

    def taken(k, carry):
        slot = k + excess - SHIFT_MOST

        @pl.when(slot >= 0)
        def _():
            emit(moved[k], slot)

        return carry

    lax.fori_loop(0, SHIFT_MOST, taken, jnp.int32(0))

    for slot in range(slots):
        pltpu.make_async_copy(made.at[slot], out.at[slot], out_sem.at[slot]).wait()


def convolve(info, mask, pixels, parcel, farther, below, weight, bias):
    rows, cols = mask.shape
    side = pixels.shape[0] // rows
    ch = weight.shape[2]
    wide = side * ch
    dtype = pixels.dtype
    smem = pl.BlockSpec(memory_space=pltpu.SMEM)
    vmem = pl.BlockSpec(memory_space=pltpu.VMEM)
    hbm = pl.BlockSpec(memory_space=pl.ANY)
    return pl.pallas_call(
        functools.partial(conv_kernel, rows=rows, cols=cols, side=side, ch=ch),
        in_specs=[smem, smem, hbm, vmem, vmem, vmem, vmem, vmem],
        out_specs=hbm,
        out_shape=jax.ShapeDtypeStruct((SLOTS, side, wide), dtype),
        scratch_shapes=[
            pltpu.VMEM((rows * side + 2 * GUARD, cols * wide + 2 * LANES), dtype),
            pltpu.VMEM((GUARD, cols * wide + 2 * LANES), dtype),
            pltpu.VMEM((SHIFT_MOST, side + 2 * GUARD, wide + 2 * LANES), dtype),
            pltpu.VMEM((wide // LANES + 1, side + 2 * RIM, LANES), jnp.float32),
            pltpu.VMEM((12 * ch, 2 * ch), dtype),
            pltpu.VMEM((SLOTS, side, wide), dtype),
            pltpu.SemaphoreType.DMA((rows * cols,)),
            pltpu.SemaphoreType.DMA((SLOTS,)),
        ],
    )(
        info,
        mask,
        pixels,
        parcel,
        farther,
        below,
        weight.reshape(9 * ch, ch),
        jnp.tile(bias.astype(jnp.float32), 2).reshape(1, 2 * ch),
    )


def on_device(slide_pixels, tissue_mask, conv_weight, conv_bias):
    size = lax.axis_size("row")
    device = lax.axis_index("row")
    card, first, last, parcel = prepare(tissue_mask, slide_pixels, size)
    table = lax.all_to_all(card, "row", 0, 0, tiled=True)
    up = [(i, i + 1) for i in range(size - 1)]
    up_two = [(i, i + 2) for i in range(size - 2)]
    down = [(i + 1, i) for i in range(size - 1)]
    parcel = lax.ppermute(parcel, "row", up)
    below = lax.ppermute(first, "row", down)
    farther = lax.ppermute(last, "row", up_two)
    sender = jnp.arange(size, dtype=jnp.int32)[:, None]
    lane = jnp.arange(LANES, dtype=jnp.int32)[None, :]
    wanted = jnp.where(lane == 0, sender < device, sender == device - 1)
    info = jnp.sum(jnp.where(wanted, table.reshape(size, LANES), 0), axis=0)
    info = info - jnp.where(lane[0] == 0, device * SLOTS, 0).astype(jnp.int32)
    return convolve(info, tissue_mask, slide_pixels, parcel, farther, below, conv_weight, conv_bias)


def solution(mesh):
    spread = ("slides", "row")
    return jax.shard_map(
        on_device,
        mesh=mesh,
        in_specs=(P(spread, None), P(spread, None), P(), P()),
        out_specs=P(spread, None, None),
        check_vma=False,
    )
```

```python
import functools

import jax
import jax.numpy as jnp
from jax import lax
from jax.experimental import pallas as pl
from jax.experimental.pallas import tpu as pltpu
from jax.sharding import PartitionSpec as P


SLOTS = 8
SHIFT_MOST = 2
LANES = 128
GUARD = 16
RIM = 8
ROOM = pltpu.CompilerParams(vmem_limit_bytes=16 * 2**20)


def fetch_band(mask, pixels, band, sem, *, rows, cols, side, wide, guard):
    def fetch(t):
        row, col = t // cols, t % cols
        return pltpu.make_async_copy(
            pixels.at[pl.ds(row * side, side), pl.ds(col * wide, wide)],
            band.at[pl.ds(guard + row * side, side), pl.ds(LANES + col * wide, wide)],
            sem.at[t],
        )

    for t in range(rows * cols):
        row, col = t // cols, t % cols

        @pl.when(mask[row, col] == 1)
        def _():
            fetch(t).start()

    for t in range(rows * cols):
        row, col = t // cols, t % cols

        @pl.when(mask[row, col] != 1)
        def _():
            band[guard + row * side : guard + (row + 1) * side, LANES + col * wide : LANES + (col + 1) * wide] = (
                jnp.zeros((side, wide), band.dtype)
            )

    edge = jnp.zeros((band.shape[0], LANES), band.dtype)
    band[:, 0:LANES] = edge
    band[:, LANES + cols * wide :] = edge

    def wait():
        for t in range(rows * cols):

            @pl.when(mask[t // cols, t % cols] == 1)
            def _():
                fetch(t).wait()

    return wait


def prepare_kernel(mask, pixels, card, first, last, parcel, band, sem, *, rows, cols, side, wide):
    count = rows * cols
    wait = fetch_band(mask, pixels, band, sem, rows=rows, cols=cols, side=side, wide=wide, guard=0)
    total = jnp.int32(0)
    for t in range(count):
        total = total + mask[t // cols, t % cols]
    places = []
    for k in range(SHIFT_MOST):
        rank, found = jnp.int32(0), jnp.int32(0)
        for t in range(count):
            hit = (mask[t // cols, t % cols] == 1) & (rank == total - SHIFT_MOST + k)
            found = jnp.where(hit, t, found)
            rank = rank + mask[t // cols, t % cols]
        places.append((found // cols, found % cols))
    lane = lax.broadcasted_iota(jnp.int32, card.shape, 2)
    info = jnp.where(lane == 0, total, 0)
    for k, (row, col) in enumerate(places):
        info = jnp.where(lane == 1 + 2 * k, row, jnp.where(lane == 2 + 2 * k, col, info))
    card[...] = info
    wait()
    first[...] = band[0:1, LANES : LANES + cols * wide]
    last[...] = band[rows * side - 1 :, LANES : LANES + cols * wide]
    window = wide + 2 * LANES
    line = lax.broadcasted_iota(jnp.int32, (RIM, window), 0)
    per = cols // SHIFT_MOST
    for k, (row, col) in enumerate(places):
        lanes = pl.ds(pl.multiple_of(col * wide, LANES), window)
        parcel[k, 0:side] = band[pl.ds(pl.multiple_of(row * side, side), side), lanes]
        near = band[pl.ds(pl.multiple_of(side - GUARD * row, GUARD), GUARD), lanes].astype(jnp.float32)
        rim = jnp.where(row == 0, near[0:1], near[GUARD - 1 : GUARD])
        block = jnp.broadcast_to(rim, (RIM, window))
        for j in range(per):
            at = (k * per + j) * wide
            low = band[rows * side - GUARD :, at : at + window].astype(jnp.float32)[GUARD - 1 : GUARD]
            block = jnp.where(line == 1 + j, jnp.broadcast_to(low, (RIM, window)), block)
        parcel[k, side:] = block.astype(parcel.dtype)


def prepare(mask, pixels, size):
    rows, cols = mask.shape
    side = pixels.shape[0] // rows
    wide = pixels.shape[1] // cols
    dtype = pixels.dtype
    vmem = pl.BlockSpec(memory_space=pltpu.VMEM)
    return pl.pallas_call(
        functools.partial(prepare_kernel, rows=rows, cols=cols, side=side, wide=wide),
        in_specs=[pl.BlockSpec(memory_space=pltpu.SMEM), pl.BlockSpec(memory_space=pl.ANY)],
        out_specs=[vmem] * 5,
        out_shape=[
            pltpu.VMEM((size, 1, LANES), jnp.int32),
            pltpu.VMEM((1, cols * wide), dtype),
            pltpu.VMEM((1, cols * wide), dtype),
            pltpu.VMEM((SHIFT_MOST, side + RIM, wide + 2 * LANES), dtype),
            pltpu.VMEM((rows * side, cols * wide + 2 * LANES), dtype),
        ],
        scratch_shapes=[pltpu.SemaphoreType.DMA((rows * cols,))],
        compiler_params=ROOM,
    )(pltpu.with_memory_space_constraint(mask, pltpu.HBM), pltpu.with_memory_space_constraint(pixels, pltpu.HBM))


def conv_kernel(
    device, table, mask, band, parcel, farther, below, weight, bias, out,
    over, under, beyond, moved, shifted, banded, made, out_sem,
    *, rows, cols, side, ch,
):
    wide = side * ch
    window = wide + 2 * LANES
    slots = out.shape[0]

    sender = lax.broadcasted_iota(jnp.int32, table.shape, 0)
    lane = lax.broadcasted_iota(jnp.int32, table.shape, 1)
    here = device[0]
    wanted = jnp.where(lane == 0, (sender < here).astype(jnp.int32), (sender == here - 1).astype(jnp.int32))
    facts = jnp.sum(table[...] * wanted, axis=0, keepdims=True)
    place = lax.broadcasted_iota(jnp.int32, facts.shape, 1)

    def fact(k):
        return jnp.sum(jnp.where(place == k, facts, 0))

    excess = fact(0) - here * slots

    inner = pl.ds(LANES, cols * wide)
    edge = jnp.zeros((GUARD, LANES), over.dtype)
    for rim in (over, under, beyond):
        rim[:, 0:LANES] = edge
        rim[:, LANES + cols * wide :] = edge
    per = cols // SHIFT_MOST
    for col in range(cols):
        row = parcel[col // per, side : side + RIM, LANES : LANES + wide].astype(jnp.float32)
        row = row[1 + col % per : 2 + col % per]
        at = LANES + col * wide
        over[:, at : at + wide] = jnp.broadcast_to(row, (GUARD, wide)).astype(over.dtype)
    under[:, inner] = jnp.broadcast_to(below[...], (GUARD, cols * wide))
    beyond[:, inner] = jnp.broadcast_to(farther[...], (GUARD, cols * wide))

    group = 2 * LANES // ch
    taps = weight[...]
    spread = lax.broadcasted_iota(jnp.int32, (ch, 2 * LANES), 1) - lax.broadcasted_iota(jnp.int32, (ch, 2 * LANES), 0)
    spots = [
        jnp.dot(taps, (spread == at * ch).astype(taps.dtype), preferred_element_type=jnp.float32).astype(taps.dtype)
        for at in range(group)
    ]
    for v in range(3):
        for i in range(group + 2):
            block = None
            for j in range(group):
                if 0 <= i - j <= 2:
                    tap = 3 * v + i - j
                    piece = spots[j][tap * ch : (tap + 1) * ch]
                    block = piece if block is None else block + piece
            at = (v * (group + 2) + i) * ch
            banded[at : at + ch] = block

    for k in range(SHIFT_MOST):
        row, col = fact(1 + 2 * k), fact(2 + 2 * k)
        lanes = pl.ds(pl.multiple_of(col * wide, LANES), window)
        moved[k, GUARD : GUARD + side] = parcel[k, 0:side]
        rim = parcel[k, side : side + RIM].astype(jnp.float32)[0:1]
        rim = jnp.broadcast_to(rim, (GUARD, window)).astype(moved.dtype)

        @pl.when(row == 0)
        def _():
            moved[k, 0:GUARD] = beyond[:, lanes]
            moved[k, GUARD + side :] = rim

        @pl.when(row != 0)
        def _():
            moved[k, 0:GUARD] = rim
            moved[k, GUARD + side :] = band[0:GUARD, lanes]

    blocks = wide // LANES + 1
    step = 2 * LANES

    def emit(top, middle, bottom, slot):
        inside = slice(LANES // 2, LANES // 2 + blocks * LANES)
        top = top[:, inside].astype(jnp.float32)[GUARD - RIM :]
        middle = middle[:, inside].astype(jnp.float32)
        bottom = bottom[:, inside].astype(jnp.float32)[:RIM]
        for q in range(blocks):
            lanes = slice(q * LANES, (q + 1) * LANES)
            shifted[q, 0:RIM] = top[:, lanes]
            shifted[q, RIM : RIM + side] = middle[:, lanes]
            shifted[q, RIM + side :] = bottom[:, lanes]
        parts = [
            [shifted[q, RIM + v - 1 : RIM + v - 1 + side].astype(out.dtype) for q in range(blocks)] for v in range(3)
        ]
        left = jnp.concatenate(
            [
                jnp.concatenate([parts[v][q + n] for v in range(3) for n in range(3)], axis=1)
                for q in range(0, blocks - 1, 2)
            ],
            axis=0,
        )
        result = jnp.dot(left, banded[...], preferred_element_type=jnp.float32)
        result = (result + bias[...]).astype(out.dtype)
        for g in range((blocks - 1) // 2):
            made[slot, :, g * step : (g + 1) * step] = result[g * side : (g + 1) * side]
        pltpu.make_async_copy(made.at[slot], out.at[slot], out_sem.at[slot]).start()

    rank = jnp.int32(0)
    for row in range(rows):

        def own(col, rank):
            slot = rank + excess

            @pl.when((mask[row, col] == 1) & (slot < slots))
            def _():
                lanes = pl.ds(pl.multiple_of(col * wide, LANES), window)
                top = over if row == 0 else band.at[row * side - GUARD : row * side]
                bottom = under if row == rows - 1 else band.at[(row + 1) * side : (row + 1) * side + GUARD]
                emit(top[:, lanes], band[row * side : (row + 1) * side, lanes], bottom[:, lanes], slot)

            return rank + mask[row, col]

        rank = lax.fori_loop(0, cols, own, rank)

    def taken(k, carry):
        slot = k + excess - SHIFT_MOST

        @pl.when(slot >= 0)
        def _():
            emit(moved[k, 0:GUARD], moved[k, GUARD : GUARD + side], moved[k, GUARD + side :], slot)

        return carry

    lax.fori_loop(0, SHIFT_MOST, taken, jnp.int32(0))

    for slot in range(slots):
        pltpu.make_async_copy(made.at[slot], out.at[slot], out_sem.at[slot]).wait()


def convolve(device, table, mask, band, parcel, farther, below, weight, bias):
    rows, cols = mask.shape
    side = band.shape[0] // rows
    ch = weight.shape[2]
    wide = side * ch
    dtype = band.dtype
    smem = pl.BlockSpec(memory_space=pltpu.SMEM)
    vmem = pl.BlockSpec(memory_space=pltpu.VMEM)
    hbm = pl.BlockSpec(memory_space=pl.ANY)
    rims = [pltpu.VMEM((GUARD, cols * wide + 2 * LANES), dtype)] * 3
    group = 2 * LANES // ch
    near = [
        table,
        band,
        parcel,
        farther,
        below,
        weight.reshape(9 * ch, ch),
        jnp.tile(bias.astype(jnp.float32), group).reshape(1, 2 * LANES),
    ]
    table, band, parcel, farther, below, weight, bias = (
        pltpu.with_memory_space_constraint(a, pltpu.VMEM) for a in near
    )
    return pl.pallas_call(
        functools.partial(conv_kernel, rows=rows, cols=cols, side=side, ch=ch),
        in_specs=[smem, vmem, smem, vmem, vmem, vmem, vmem, vmem, vmem],
        out_specs=hbm,
        out_shape=jax.ShapeDtypeStruct((SLOTS, side, wide), dtype),
        scratch_shapes=[
            *rims,
            pltpu.VMEM((SHIFT_MOST, side + 2 * GUARD, wide + 2 * LANES), dtype),
            pltpu.VMEM((wide // LANES + 1, side + 2 * RIM, LANES), jnp.float32),
            pltpu.VMEM((3 * (group + 2) * ch, 2 * LANES), dtype),
            pltpu.VMEM((SLOTS, side, wide), dtype),
            pltpu.SemaphoreType.DMA((SLOTS,)),
        ],
        compiler_params=ROOM,
    )(device, table, pltpu.with_memory_space_constraint(mask, pltpu.HBM), band, parcel, farther, below, weight, bias)


def on_device(slide_pixels, tissue_mask, conv_weight, conv_bias):
    size = lax.axis_size("row")
    device = lax.axis_index("row").astype(jnp.int32).reshape(1)
    card, first, last, parcel, band = prepare(tissue_mask, slide_pixels, size)
    up = [(i, i + 1) for i in range(size - 1)]
    up_two = [(i, i + 2) for i in range(size - 2)]
    down = [(i + 1, i) for i in range(size - 1)]
    parcel = lax.ppermute(parcel, "row", up)
    table = lax.all_to_all(card, "row", 0, 0, tiled=True)
    below = lax.ppermute(first, "row", down)
    farther = lax.ppermute(last, "row", up_two)
    table = table.reshape(size, LANES)
    return convolve(device, table, tissue_mask, band, parcel, farther, below, conv_weight, conv_bias)


def solution(mesh):
    spread = ("slides", "row")
    return jax.shard_map(
        on_device,
        mesh=mesh,
        in_specs=(P(spread, None), P(spread, None), P(), P()),
        out_specs=P(spread, None, None),
        check_vma=False,
    )
```
